32 devices in a mesh: tok: 8 (over y, x, core), blk: 4 (over z).
Axes of the slice: x: 2, y: 2, z: 4, core: 2. Of those that a mesh axis runs over, the one named last changes fastest.
Arguments:
- activations: bfloat16 [4096, 4096], P('tok', 'blk'), may hold values from -52 to 52, as said below
- out_grads: bfloat16 [4096, 4096], P('tok', 'blk'), may hold values from -52 to 52, as said below
Outputs:
- act_inverse: float32 [4096, 4096], P(('tok', 'blk'))
- grad_inverse: float32 [4096, 4096], P(('tok', 'blk'))
The draws below stay inside these ranges and needn't reach their ends.
Inputs may be any that keep to these rules, and one draw needn't show every extreme that they name: `activations`: real entries. `out_grads`: real entries.
All inputs are finite; a program needn't handle non-finite values.
Results may differ from the reference program's by a relative error of at most 0.02.
Values may be sent and summed in bfloat16 or wider, within the bound.
A program may use at most 64 MiB of HBM per device.

```python
import jax
import jax.numpy as jnp
from jax import lax

D = 4096
TOK_DEV = 512
TOKENS = 4096
N_TOK = 8


def scaled_draw(key):
    row_key, col_key, value_key = jax.random.split(key, 3)
    positions = jnp.arange(TOKENS, dtype=jnp.float32) / TOKENS
    values = jax.random.truncated_normal(value_key, -5.0, 5.0, (TOKENS, D), jnp.float32)
    row_scale = jnp.exp(jax.random.uniform(row_key, (TOKENS, 1), jnp.float32, 0.0, jnp.log(3.0)))
    ramp = jnp.exp(positions * 0.5 * jnp.log(3.0))
    col_scale = jnp.exp(jax.random.uniform(col_key, (1, D), jnp.float32, 0.0, jnp.log(10.0)))
    return values * row_scale * ramp[:, None] * col_scale / 10.0


def draw_activations(key, part):
    return scaled_draw(jax.random.fold_in(key, 11)).astype(jnp.bfloat16)


def draw_out_grads(key, part):
    return scaled_draw(jax.random.fold_in(key, 23)).astype(jnp.bfloat16)


def setup_inputs(seed: int = 0) -> dict:
    streams_of = jax.random.split(jax.random.key(seed), 3)
    activations = draw_activations(jax.random.fold_in(streams_of[2], 71), 0)
    out_grads = draw_out_grads(jax.random.fold_in(streams_of[2], 71), 0)
    return dict(activations=activations, out_grads=out_grads)


damping = 0.3
epsilon = 1e-06
divisor = 2.0

def factor_gram(data):
    shards = data.reshape(N_TOK, TOK_DEV, D)

    def add_shard(total, shard):
        partial_value = jnp.dot(shard.T, shard, preferred_element_type=jnp.float32)
        rounded = lax.optimization_barrier(partial_value.astype(jnp.bfloat16))
        return (total + rounded.astype(jnp.float32), None)
    total, unused = lax.scan(add_shard, jnp.zeros((D, D), jnp.float32), shards)
    return total

def factor_inverse(data):
    gram = factor_gram(data)
    values = data.astype(jnp.float32)
    sums = lax.optimization_barrier(jnp.sum(values * values, axis=0))
    inverse = lax.rsqrt(sums / TOKENS + epsilon)
    identity = jnp.eye(D, dtype=jnp.float32)
    damped = gram / TOKENS * inverse[:, None] * inverse[None, :] + damping * identity
    scaled = damped / divisor
    half = scaled.astype(jnp.bfloat16)
    square = jnp.dot(half, half, preferred_element_type=jnp.float32)
    cube = jnp.dot(half, square.astype(jnp.bfloat16), preferred_element_type=jnp.float32)
    return 4.0 * identity - 6.0 * scaled + 4.0 * square - cube

def reference(activations, out_grads):
    return (factor_inverse(activations), factor_inverse(out_grads))
```

```python
import functools

import jax
import jax.numpy as jnp
from jax import lax
from jax.experimental import pallas as pl
from jax.experimental.pallas import tpu as pltpu
from jax.sharding import PartitionSpec as P

damping = 0.3
epsilon = 1e-06
divisor = 2.0
gathered_budget = 32 * 1024 * 1024
MESH = pl.DeviceIdType.MESH


def column_squares(data):
    values = data.astype(jnp.float32)
    return jnp.sum(values * values, axis=0)


def fold_product(row_block, tile):
    return jnp.dot(
        row_block,
        lax.all_gather(tile, "tok", axis=0, tiled=True),
        preferred_element_type=jnp.float32,
    )


def newton_steps(scaled, identity):
    half = scaled.astype(jnp.bfloat16)
    row_block = lax.all_gather(half, "blk", axis=1, tiled=True)
    square = fold_product(row_block, half)
    cube = fold_product(row_block, square.astype(jnp.bfloat16))
    return 4.0 * identity - 6.0 * scaled + 4.0 * square - cube


def tiled_body(activations, out_grads):
    tok_count = lax.axis_size("tok")
    blk_count = lax.axis_size("blk")
    tok_id = lax.axis_index("tok")
    blk_id = lax.axis_index("blk")
    token_count = activations.shape[0] * tok_count
    tile_cols = activations.shape[1]
    tile_rows = tile_cols * blk_count // tok_count
    row_ids = tok_id * tile_rows + jnp.arange(tile_rows, dtype=jnp.int32)
    col_ids = blk_id * tile_cols + jnp.arange(tile_cols, dtype=jnp.int32)
    identity = (row_ids[:, None] == col_ids[None, :]).astype(jnp.float32)

    def inverse_tile(local):
        full = lax.all_gather(local, "blk", axis=1, tiled=True)
        sums = lax.psum(column_squares(full).astype(jnp.bfloat16), "tok").astype(jnp.float32)
        gram_tile = lax.psum_scatter(
            lax.dot_general(
                full, local, (((0,), (0,)), ((), ())), preferred_element_type=jnp.float32
            ).astype(jnp.bfloat16),
            "tok",
            scatter_dimension=0,
            tiled=True,
        ).astype(jnp.float32)
        inverse = lax.rsqrt(sums / token_count + epsilon)
        inverse_rows = lax.dynamic_slice_in_dim(inverse, tok_id * tile_rows, tile_rows)
        inverse_cols = lax.dynamic_slice_in_dim(inverse, blk_id * tile_cols, tile_cols)
        damped = (
            gram_tile / token_count * inverse_rows[:, None] * inverse_cols[None, :]
            + damping * identity
        )
        result_tile = newton_steps(damped / divisor, identity)
        return lax.all_to_all(
            result_tile.astype(jnp.bfloat16), "blk", split_axis=0, concat_axis=1, tiled=True
        ).astype(result_tile.dtype)

    return inverse_tile(activations), inverse_tile(out_grads)


def cut(length, unit, pieces):
    units = length // unit
    sizes = [(units // pieces + (1 if i < units % pieces else 0)) * unit for i in range(pieces)]
    return [(sum(sizes[:i]), sizes[i]) for i in range(pieces)]


def gather_kernel(tok, blk, swaps, block_shape, *refs):
    first, second, out, send_sem, recv_sem, pass_send, pass_recv, swap_send, swap_recv, local_sem = refs
    t = lax.axis_index("tok")
    b = lax.axis_index("blk")
    half = blk // 2
    dims = []
    bit = 2
    while bit < tok:
        dims.append((bit, 0))
        bit *= 2
    bit = 1
    while bit < half:
        dims.append((0, bit))
        bit *= 2
    count = len(dims)
    rows, cols = block_shape
    if swaps:
        parts = [((o, n), (0, cols)) for o, n in cut(rows, 16, count)]
    else:
        parts = [((0, rows), (o, n)) for o, n in cut(cols, 128, count)]

    def flip(j, steps, tok_bits=0, blk_bits=0):
        for s in range(count):
            if steps >> s & 1:
                dt, db = dims[(j + s) % count]
                tok_bits ^= dt
                blk_bits ^= db
        return jnp.bitwise_xor(t, tok_bits), jnp.bitwise_xor(b, blk_bits)

    def place(q, part, owner):
        (r0, rn), (c0, cn) = parts[part]
        tt, bb = owner
        if q:
            bb = jnp.bitwise_xor(bb, half)
        if swaps:
            row, col = tt * rows + r0, bb * cols + c0
        else:
            row, col = (tt * blk + bb) * rows + r0, c0
        return out.at[
            pl.ds(pl.multiple_of(row, 16), rn), pl.ds(pl.multiple_of(col, 128), cn)
        ]

    def own(q, part):
        (r0, rn), (c0, cn) = parts[part]
        if q and swaps:
            return place(q, part, (t, b))
        return (second if q else first).at[pl.ds(r0, rn), pl.ds(c0, cn)]

    def hop(q, j, steps, s):
        src = own(q, j) if steps == 0 else place(q, j, flip(j, steps))
        index = (q * count + j) * 2**count + (steps | 1 << s)
        return pltpu.make_async_remote_copy(
            src_ref=src,
            dst_ref=place(q, j, flip(j, steps)),
            send_sem=send_sem.at[index],
            recv_sem=recv_sem.at[index],
            device_id=flip(j, 1 << s),
            device_id_type=MESH,
        )

    def arrival(q, j, steps):
        index = (q * count + j) * 2**count + steps
        where = place(q, j, flip(j, steps))
        return pltpu.make_async_remote_copy(
            src_ref=where,
            dst_ref=where,
            send_sem=send_sem.at[index],
            recv_sem=recv_sem.at[index],
            device_id=flip(j, 1),
            device_id_type=MESH,
        )

    def handed(q, j, steps, sender):
        index = (q * count + j) * 2**count + steps
        if sender:
            where = place(q, j, flip(j, steps))
            src = own(q, j) if steps == 0 else where
        else:
            where = place(q, j, flip(j, steps, 1))
            src = where
        return pltpu.make_async_remote_copy(
            src_ref=src,
            dst_ref=where,
            send_sem=pass_send.at[index],
            recv_sem=pass_recv.at[index],
            device_id=(jnp.bitwise_xor(t, 1), b),
            device_id_type=MESH,
        )

    across = (t, jnp.bitwise_xor(b, half))

    def swap(part, sender):
        (r0, rn), (c0, cn) = parts[part]
        if sender:
            src = second.at[pl.ds(r0, rn), pl.ds(c0, cn)]
            where = place(1, part, across)
        else:
            src = where = place(1, part, (t, b))
        return pltpu.make_async_remote_copy(
            src_ref=src,
            dst_ref=where,
            send_sem=swap_send.at[part],
            recv_sem=swap_recv.at[part],
            device_id=across,
            device_id_type=MESH,
        )

    barrier = pltpu.get_barrier_semaphore()
    peers = [flip(0, 1 << s) for s in range(count)] + [(jnp.bitwise_xor(t, 1), b)]
    if swaps:
        peers.append(across)
    for peer in peers:
        pl.semaphore_signal(barrier, inc=1, device_id=peer, device_id_type=MESH)
    pl.semaphore_wait(barrier, len(peers))

    pending = []

    def start(copy):
        copy.start()
        pending.append(copy)

    def begin(q):
        for s in range(count):
            for j in range(count):
                if s == 0 and q and swaps:
                    swap(j, False).wait_recv()
                start(hop(q, j, 0, s))
        for j in range(count):
            start(handed(q, j, 0, True))

    def advance(q, p):
        for steps in range(2**p, 2 ** (p + 1)):
            for j in range(count):
                arrival(q, j, steps).wait_recv()
                for s in range(p + 1, count):
                    start(hop(q, j, steps, s))
                start(handed(q, j, steps, True))

    begin(0)
    if swaps:
        for part in range(count):
            start(swap(part, True))
    locals_ = []
    for q in range(1 if swaps else 2):
        for part in range(count):
            copy = pltpu.make_async_copy(
                own(q, part), place(q, part, (t, b)), local_sem.at[q * count + part]
            )
            copy.start()
            locals_.append(copy)
    for p in range(count - 1):
        advance(0, p)
    begin(1)
    advance(0, count - 1)
    for p in range(count):
        advance(1, p)
    for q in range(2):
        for j in range(count):
            for steps in range(2**count):
                handed(q, j, steps, False).wait_recv()
    for copy in locals_:
        copy.wait()
    for copy in pending:
        copy.wait_send()


def gather(first, second, tok, blk, swaps, full_shape, collective_id):
    count = (tok // 2).bit_length() - 1 + (blk // 2).bit_length() - 1
    slots = 2 * count * 2**count
    return pl.pallas_call(
        functools.partial(gather_kernel, tok, blk, swaps, first.shape),
        out_shape=jax.ShapeDtypeStruct(full_shape, first.dtype),
        in_specs=[pl.BlockSpec(memory_space=pltpu.VMEM)] * 2,
        out_specs=pl.BlockSpec(memory_space=pl.ANY),
        scratch_shapes=[pltpu.SemaphoreType.DMA((slots,))] * 4
        + [pltpu.SemaphoreType.DMA((count,))] * 2
        + [pltpu.SemaphoreType.DMA((2 * count,))],
        compiler_params=pltpu.CompilerParams(
            collective_id=collective_id, has_side_effects=True, vmem_limit_bytes=16 * 1024 * 1024
        ),
        cost_estimate=pl.CostEstimate(
            flops=0, bytes_accessed=2 * full_shape[0] * full_shape[1] * 16, transcendentals=0
        ),
    )(first, second)


def split_body(tok, blk, activations, out_grads):
    half = blk // 2
    t = lax.axis_index("tok")
    b = lax.axis_index("blk")
    tokens = activations.shape[0] * tok
    width = activations.shape[1] * blk
    rows = width // (tok * blk)
    low = b < half
    mine = jnp.where(low, activations, out_grads)
    other = jnp.where(low, out_grads, activations)

    partial_sums = jnp.stack([column_squares(activations), column_squares(out_grads)])
    all_sums = lax.all_gather(partial_sums, ("tok", "blk"), axis=0, tiled=False)
    both = all_sums.reshape(tok, blk, 2, -1).sum(axis=0).transpose(1, 0, 2).reshape(2, width)
    sums = jnp.where(low, both[0], both[1])
    inverse = lax.rsqrt(sums / tokens + epsilon)

    x = gather(mine, other, tok, blk, True, (tokens, width), 0)
    starts = [(t * blk + b) * rows, (t * blk + jnp.bitwise_xor(b, half)) * rows]
    x_own = jnp.concatenate(
        [lax.dynamic_slice_in_dim(x, s, rows, axis=1) for s in starts], axis=1
    )
    inverse_own = jnp.concatenate([lax.dynamic_slice_in_dim(inverse, s, rows) for s in starts])
    gram = lax.dot_general(x_own, x, (((0,), (0,)), ((), ())), preferred_element_type=jnp.float32)
    row_ids = jnp.concatenate([s + jnp.arange(rows, dtype=jnp.int32) for s in starts])
    identity = (row_ids[:, None] == jnp.arange(width, dtype=jnp.int32)[None, :]).astype(jnp.float32)
    scaled = (
        gram / tokens * inverse_own[:, None] * inverse[None, :] + damping * identity
    ) / divisor
    h_own = scaled.astype(jnp.bfloat16)
    h = gather(h_own[:rows], h_own[rows:], tok, blk, False, (width, width), 1)
    square = jnp.dot(h_own, h, preferred_element_type=jnp.float32)
    cube = jnp.dot(square.astype(jnp.bfloat16), h, preferred_element_type=jnp.float32)
    result = 4.0 * identity - 6.0 * scaled + 4.0 * square - cube
    kept = result[:rows]
    came = lax.ppermute(
        result[rows:].astype(jnp.bfloat16), "blk", [(i, i ^ half) for i in range(blk)]
    ).astype(jnp.float32)
    return jnp.where(low, kept, came), jnp.where(low, came, kept)


def solution(mesh):
    tok, blk = mesh.shape["tok"], mesh.shape["blk"]
    placed = (P("tok", "blk"), P("tok", "blk"))

    def body(activations, out_grads):
        tokens, width = activations.shape[0] * tok, activations.shape[1] * blk
        whole = max(tokens, width) * width * activations.dtype.itemsize
        powers = tok & (tok - 1) == 0 and blk & (blk - 1) == 0 and tok > 2 and blk > 1
        if whole <= gathered_budget and powers:
            return split_body(tok, blk, activations, out_grads)
        return tiled_body(activations, out_grads)

    return jax.shard_map(
        body,
        mesh=mesh,
        in_specs=placed,
        out_specs=(P(("tok", "blk"), None), P(("tok", "blk"), None)),
        check_vma=False,
    )
```

```python
import functools

import jax
import jax.numpy as jnp
from jax import lax
from jax.experimental import pallas as pl
from jax.experimental.pallas import tpu as pltpu
from jax.sharding import PartitionSpec as P

damping = 0.3
epsilon = 1e-06
divisor = 2.0
gathered_budget = 32 * 1024 * 1024
LANES = 128
CHUNK = 512
MESH = pl.DeviceIdType.MESH


def column_squares(data):
    values = data.astype(jnp.float32)
    return jnp.sum(values * values, axis=0)


def fold_product(row_block, tile):
    return jnp.dot(
        row_block,
        lax.all_gather(tile, "tok", axis=0, tiled=True),
        preferred_element_type=jnp.float32,
    )


def newton_steps(scaled, identity):
    half = scaled.astype(jnp.bfloat16)
    row_block = lax.all_gather(half, "blk", axis=1, tiled=True)
    square = fold_product(row_block, half)
    cube = fold_product(row_block, square.astype(jnp.bfloat16))
    return 4.0 * identity - 6.0 * scaled + 4.0 * square - cube


def tiled_body(activations, out_grads):
    tok_count = lax.axis_size("tok")
    blk_count = lax.axis_size("blk")
    tok_id = lax.axis_index("tok")
    blk_id = lax.axis_index("blk")
    token_count = activations.shape[0] * tok_count
    tile_cols = activations.shape[1]
    tile_rows = tile_cols * blk_count // tok_count
    row_ids = tok_id * tile_rows + jnp.arange(tile_rows, dtype=jnp.int32)
    col_ids = blk_id * tile_cols + jnp.arange(tile_cols, dtype=jnp.int32)
    identity = (row_ids[:, None] == col_ids[None, :]).astype(jnp.float32)

    def inverse_tile(local):
        full = lax.all_gather(local, "blk", axis=1, tiled=True)
        sums = lax.psum(column_squares(full).astype(jnp.bfloat16), "tok").astype(jnp.float32)
        gram_tile = lax.psum_scatter(
            lax.dot_general(
                full, local, (((0,), (0,)), ((), ())), preferred_element_type=jnp.float32
            ).astype(jnp.bfloat16),
            "tok",
            scatter_dimension=0,
            tiled=True,
        ).astype(jnp.float32)
        inverse = lax.rsqrt(sums / token_count + epsilon)
        inverse_rows = lax.dynamic_slice_in_dim(inverse, tok_id * tile_rows, tile_rows)
        inverse_cols = lax.dynamic_slice_in_dim(inverse, blk_id * tile_cols, tile_cols)
        damped = (
            gram_tile / token_count * inverse_rows[:, None] * inverse_cols[None, :]
            + damping * identity
        )
        result_tile = newton_steps(damped / divisor, identity)
        return lax.all_to_all(
            result_tile.astype(jnp.bfloat16), "blk", split_axis=0, concat_axis=1, tiled=True
        ).astype(result_tile.dtype)

    return inverse_tile(activations), inverse_tile(out_grads)


def cut(length, unit, pieces):
    units = length // unit
    sizes = [(units // pieces + (1 if i < units % pieces else 0)) * unit for i in range(pieces)]
    return [(sum(sizes[:i]), sizes[i]) for i in range(pieces)]


def gather_blocks(tok, blk, swaps, first, second, out, sems):
    send_sem, recv_sem, pass_send, pass_recv, swap_send, swap_recv, local_sem = sems
    t = lax.axis_index("tok")
    b = lax.axis_index("blk")
    half = blk // 2
    dims = []
    bit = 2
    while bit < tok:
        dims.append((bit, 0))
        bit *= 2
    bit = 1
    while bit < half:
        dims.append((0, bit))
        bit *= 2
    count = len(dims)
    rows, cols = first.shape
    if swaps:
        parts = [((o, n), (0, cols)) for o, n in cut(rows, 16, count)]
    else:
        parts = [((0, rows), (o, n)) for o, n in cut(cols, 128, count)]

    def flip(j, steps, tok_bits=0, blk_bits=0):
        for s in range(count):
            if steps >> s & 1:
                dt, db = dims[(j + s) % count]
                tok_bits ^= dt
                blk_bits ^= db
        return jnp.bitwise_xor(t, tok_bits), jnp.bitwise_xor(b, blk_bits)

    def place(q, part, owner):
        (r0, rn), (c0, cn) = parts[part]
        tt, bb = owner
        if q:
            bb = jnp.bitwise_xor(bb, half)
        if swaps:
            row, col = tt * rows + r0, bb * cols + c0
        else:
            row, col = (tt * blk + bb) * rows + r0, c0
        return out.at[
            pl.ds(pl.multiple_of(row, 16), rn), pl.ds(pl.multiple_of(col, 128), cn)
        ]

    def own(q, part):
        (r0, rn), (c0, cn) = parts[part]
        if q and swaps:
            return place(q, part, (t, b))
        return (second if q else first).at[pl.ds(r0, rn), pl.ds(c0, cn)]

    def hop(q, j, steps, s):
        src = own(q, j) if steps == 0 else place(q, j, flip(j, steps))
        index = (q * count + j) * 2**count + (steps | 1 << s)
        return pltpu.make_async_remote_copy(
            src_ref=src,
            dst_ref=place(q, j, flip(j, steps)),
            send_sem=send_sem.at[index],
            recv_sem=recv_sem.at[index],
            device_id=flip(j, 1 << s),
            device_id_type=MESH,
        )

    def arrival(q, j, steps):
        index = (q * count + j) * 2**count + steps
        where = place(q, j, flip(j, steps))
        return pltpu.make_async_remote_copy(
            src_ref=where,
            dst_ref=where,
            send_sem=send_sem.at[index],
            recv_sem=recv_sem.at[index],
            device_id=flip(j, 1),
            device_id_type=MESH,
        )

    def handed(q, j, steps, sender):
        index = (q * count + j) * 2**count + steps
        if sender:
            where = place(q, j, flip(j, steps))
            src = own(q, j) if steps == 0 else where
        else:
            where = place(q, j, flip(j, steps, 1))
            src = where
        return pltpu.make_async_remote_copy(
            src_ref=src,
            dst_ref=where,
            send_sem=pass_send.at[index],
            recv_sem=pass_recv.at[index],
            device_id=(jnp.bitwise_xor(t, 1), b),
            device_id_type=MESH,
        )

    across = (t, jnp.bitwise_xor(b, half))

    def swap(part, sender):
        (r0, rn), (c0, cn) = parts[part]
        if sender:
            src = second.at[pl.ds(r0, rn), pl.ds(c0, cn)]
            where = place(1, part, across)
        else:
            src = where = place(1, part, (t, b))
        return pltpu.make_async_remote_copy(
            src_ref=src,
            dst_ref=where,
            send_sem=swap_send.at[part],
            recv_sem=swap_recv.at[part],
            device_id=across,
            device_id_type=MESH,
        )

    barrier = pltpu.get_barrier_semaphore()
    peers = [flip(0, 1 << s) for s in range(count)] + [(jnp.bitwise_xor(t, 1), b), across]
    for peer in peers:
        pl.semaphore_signal(barrier, inc=1, device_id=peer, device_id_type=MESH)
    pl.semaphore_wait(barrier, len(peers))

    pending = []

    def start(copy):
        copy.start()
        pending.append(copy)

    def begin(q):
        for s in range(count):
            for j in range(count):
                if s == 0 and q and swaps:
                    swap(j, False).wait_recv()
                start(hop(q, j, 0, s))
        for j in range(count):
            start(handed(q, j, 0, True))

    def advance(q, p):
        for steps in range(2**p, 2 ** (p + 1)):
            for j in range(count):
                arrival(q, j, steps).wait_recv()
                for s in range(p + 1, count):
                    start(hop(q, j, steps, s))
                start(handed(q, j, steps, True))

    begin(0)
    if swaps:
        for part in range(count):
            start(swap(part, True))
    locals_ = []
    for q in range(1 if swaps else 2):
        for part in range(count):
            copy = pltpu.make_async_copy(
                own(q, part), place(q, part, (t, b)), local_sem.at[q * count + part]
            )
            copy.start()
            locals_.append(copy)
    for p in range(count - 1):
        advance(0, p)
    begin(1)
    advance(0, count - 1)
    for p in range(count):
        advance(1, p)
    for q in range(2):
        for j in range(count):
            for steps in range(2**count):
                handed(q, j, steps, False).wait_recv()
    for copy in locals_:
        copy.wait()
    for copy in pending:
        copy.wait_send()


def gather_scratch(tok, blk):
    count = (tok // 2).bit_length() - 1 + (blk // 2).bit_length() - 1
    slots = 2 * count * 2**count
    return (
        [pltpu.SemaphoreType.DMA((slots,))] * 4
        + [pltpu.SemaphoreType.DMA((count,))] * 2
        + [pltpu.SemaphoreType.DMA((2 * count,))]
    )


def row_starts(tok, blk, rows):
    t = lax.axis_index("tok")
    b = lax.axis_index("blk")
    return [
        pl.multiple_of((t * blk + bb) * rows, LANES) for bb in (b, jnp.bitwise_xor(b, blk // 2))
    ]


def gram_kernel(tok, blk, first, second, gram, rounded, x, turned, *sems):
    tokens, width = x.shape
    rows = width // (tok * blk)
    gather_blocks(tok, blk, True, first, second, x, sems)
    step = first.shape[0]
    for s, start in enumerate(row_starts(tok, blk, rows)):

        @pl.loop(0, tokens // step)
        def _(i):
            at = pl.ds(pl.multiple_of(i * step, step), step)
            turned[s * rows : (s + 1) * rows, at] = x[at, pl.ds(start, rows)].T

    @pl.loop(0, width // CHUNK)
    def _(i):
        at = pl.ds(pl.multiple_of(i * CHUNK, CHUNK), CHUNK)
        product = jnp.dot(turned[...], x[:, at], preferred_element_type=jnp.float32)
        gram[:, at] = product
        rounded[:, at] = product.astype(jnp.bfloat16)


def newton_kernel(
    tok, blk, tokens, first, second, gram, kept, came, g, square, left, inverse, sent,
    out_sem, in_sem, *sems
):
    width = g.shape[1]
    rows = width // (tok * blk)
    t = lax.axis_index("tok")
    b = lax.axis_index("blk")
    starts = row_starts(tok, blk, rows)
    gather_blocks(tok, blk, False, first, second, g, sems)
    factor = 1.0 / (tokens * divisor)
    shift = damping / divisor
    eye = lax.broadcasted_iota(jnp.int32, (LANES, LANES), 0) == lax.broadcasted_iota(
        jnp.int32, (LANES, LANES), 1
    )

    @pl.loop(0, width // LANES)
    def _(i):
        at = pl.ds(pl.multiple_of(i * LANES, LANES), LANES)
        block = jnp.where(eye, g[at, at].astype(jnp.float32), 0.0)
        inverse[:, at] = lax.rsqrt(jnp.sum(block, axis=0, keepdims=True) / tokens + epsilon)

    inverse_rows = []
    for s, start in enumerate(starts):
        parts = []
        for r in range(0, rows, LANES):
            own = gram[s * rows + r : s * rows + r + LANES, pl.ds(start + r, LANES)]
            total = jnp.sum(jnp.where(eye, own, 0.0), axis=1, keepdims=True)
            parts.append(lax.rsqrt(total / tokens + epsilon))
        inverse_rows += parts
    inverse_rows = jnp.concatenate(inverse_rows, axis=0)

    def identity(i):
        col = i * CHUNK + lax.broadcasted_iota(jnp.int32, (rows, CHUNK), 1)
        row = lax.broadcasted_iota(jnp.int32, (rows, CHUNK), 0)
        return jnp.concatenate(
            [(col - start == row).astype(jnp.float32) for start in starts], axis=0
        )

    def scaled(i, at):
        return gram[:, at] * factor * inverse_rows * inverse[:, at] + shift * identity(i)

    @pl.loop(0, width // CHUNK)
    def _(i):
        at = pl.ds(pl.multiple_of(i * CHUNK, CHUNK), CHUNK)
        left[:, at] = (scaled(i, at) * inverse[:, at]).astype(jnp.bfloat16)

    @pl.loop(0, width // CHUNK)
    def _(i):
        at = pl.ds(pl.multiple_of(i * CHUNK, CHUNK), CHUNK)
        product = jnp.dot(left[...], g[:, at], preferred_element_type=jnp.float32)
        square[:, at] = product * (inverse[:, at] * factor) + shift * scaled(i, at)

    @pl.loop(0, width // CHUNK)
    def _(i):
        at = pl.ds(pl.multiple_of(i * CHUNK, CHUNK), CHUNK)
        left[:, at] = (square[:, at] * inverse[:, at]).astype(jnp.bfloat16)

    def swap(i):
        at = pl.ds(pl.multiple_of(i * CHUNK, CHUNK), CHUNK)
        return pltpu.make_async_remote_copy(
            src_ref=sent.at[:, at],
            dst_ref=came.at[:, at],
            send_sem=out_sem.at[i],
            recv_sem=in_sem.at[i],
            device_id=(t, jnp.bitwise_xor(b, blk // 2)),
            device_id_type=MESH,
        )

    steps = width // CHUNK

    def finish(i):
        at = pl.ds(pl.multiple_of(i * CHUNK, CHUNK), CHUNK)
        product = jnp.dot(left[...], g[:, at], preferred_element_type=jnp.float32)
        squared = square[:, at]
        cube = product * (inverse[:, at] * factor) + shift * squared
        result = 4.0 * identity(i) - 6.0 * scaled(i, at) + 4.0 * squared - cube
        kept[:, at] = result[:rows]
        sent[:, at] = result[rows:].astype(jnp.bfloat16)

    finish(0)

    @pl.loop(1, steps)
    def _(i):
        finish(i)
        swap(i - 1).start()

    swap(steps - 1).start()

    @pl.loop(0, steps)
    def _(i):
        swap(i).wait_recv()
        swap(i).wait_send()


def call(kernel, outs, scratch, tok, blk, collective_id, *operands):
    return pl.pallas_call(
        kernel,
        out_shape=outs,
        in_specs=[pl.BlockSpec(memory_space=pltpu.VMEM)] * len(operands),
        out_specs=[pl.BlockSpec(memory_space=pltpu.VMEM)] * len(outs),
        scratch_shapes=scratch + gather_scratch(tok, blk),
        compiler_params=pltpu.CompilerParams(
            collective_id=collective_id, has_side_effects=True, vmem_limit_bytes=60 * 1024 * 1024
        ),
    )(*operands)


def split_body(tok, blk, activations, out_grads):
    tokens = activations.shape[0] * tok
    width = activations.shape[1] * blk
    rows = width // (tok * blk)
    low = lax.axis_index("blk") < blk // 2
    mine = jnp.where(low, activations, out_grads)
    other = jnp.where(low, out_grads, activations)
    steps = width // CHUNK
    gram, rounded = call(
        functools.partial(gram_kernel, tok, blk),
        [
            jax.ShapeDtypeStruct((2 * rows, width), jnp.float32),
            jax.ShapeDtypeStruct((2 * rows, width), jnp.bfloat16),
        ],
        [
            pltpu.VMEM((tokens, width), jnp.bfloat16),
            pltpu.VMEM((2 * rows, tokens), jnp.bfloat16),
        ],
        tok, blk, 0, mine, other,
    )
    kept, came = call(
        functools.partial(newton_kernel, tok, blk, tokens),
        [
            jax.ShapeDtypeStruct((rows, width), jnp.float32),
            jax.ShapeDtypeStruct((rows, width), jnp.bfloat16),
        ],
        [
            pltpu.VMEM((width, width), jnp.bfloat16),
            pltpu.VMEM((2 * rows, width), jnp.float32),
            pltpu.VMEM((2 * rows, width), jnp.bfloat16),
            pltpu.VMEM((1, width), jnp.float32),
            pltpu.VMEM((rows, width), jnp.bfloat16),
            pltpu.SemaphoreType.DMA((steps,)),
            pltpu.SemaphoreType.DMA((steps,)),
        ],
        tok, blk, 1, rounded[:rows], rounded[rows:], gram,
    )
    came = came.astype(jnp.float32)
    return jnp.where(low, kept, came), jnp.where(low, came, kept)


def solution(mesh):
    tok, blk = mesh.shape["tok"], mesh.shape["blk"]
    placed = (P("tok", "blk"), P("tok", "blk"))

    def body(activations, out_grads):
        tokens, width = activations.shape[0] * tok, activations.shape[1] * blk
        whole = max(tokens, width) * width * activations.dtype.itemsize
        powers = tok & (tok - 1) == 0 and blk & (blk - 1) == 0 and tok > 2 and blk > 1
        powers = powers and width % (tok * blk * LANES) == 0
        if whole <= gathered_budget and powers:
            return split_body(tok, blk, activations, out_grads)
        return tiled_body(activations, out_grads)

    return jax.shard_map(
        body,
        mesh=mesh,
        in_specs=placed,
        out_specs=(P(("tok", "blk"), None), P(("tok", "blk"), None)),
        check_vma=False,
    )
```

```python
import functools

import jax
import jax.numpy as jnp
import numpy as np
from jax import lax
from jax.experimental import pallas as pl
from jax.experimental.pallas import tpu as pltpu
from jax.sharding import PartitionSpec as P

damping = 0.3
epsilon = 1e-06
divisor = 2.0
gathered_budget = 32 * 1024 * 1024
LANES = 128
CHUNK = 512
MESH = pl.DeviceIdType.MESH


def column_squares(data):
    values = data.astype(jnp.float32)
    return jnp.sum(values * values, axis=0)


def fold_product(row_block, tile):
    return jnp.dot(
        row_block,
        lax.all_gather(tile, "tok", axis=0, tiled=True),
        preferred_element_type=jnp.float32,
    )


def newton_steps(scaled, identity):
    half = scaled.astype(jnp.bfloat16)
    row_block = lax.all_gather(half, "blk", axis=1, tiled=True)
    square = fold_product(row_block, half)
    cube = fold_product(row_block, square.astype(jnp.bfloat16))
    return 4.0 * identity - 6.0 * scaled + 4.0 * square - cube


def tiled_body(activations, out_grads):
    tok_count = lax.axis_size("tok")
    blk_count = lax.axis_size("blk")
    tok_id = lax.axis_index("tok")
    blk_id = lax.axis_index("blk")
    token_count = activations.shape[0] * tok_count
    tile_cols = activations.shape[1]
    tile_rows = tile_cols * blk_count // tok_count
    row_ids = tok_id * tile_rows + jnp.arange(tile_rows, dtype=jnp.int32)
    col_ids = blk_id * tile_cols + jnp.arange(tile_cols, dtype=jnp.int32)
    identity = (row_ids[:, None] == col_ids[None, :]).astype(jnp.float32)

    def inverse_tile(local):
        full = lax.all_gather(local, "blk", axis=1, tiled=True)
        sums = lax.psum(column_squares(full).astype(jnp.bfloat16), "tok").astype(jnp.float32)
        gram_tile = lax.psum_scatter(
            lax.dot_general(
                full, local, (((0,), (0,)), ((), ())), preferred_element_type=jnp.float32
            ).astype(jnp.bfloat16),
            "tok",
            scatter_dimension=0,
            tiled=True,
        ).astype(jnp.float32)
        inverse = lax.rsqrt(sums / token_count + epsilon)
        inverse_rows = lax.dynamic_slice_in_dim(inverse, tok_id * tile_rows, tile_rows)
        inverse_cols = lax.dynamic_slice_in_dim(inverse, blk_id * tile_cols, tile_cols)
        damped = (
            gram_tile / token_count * inverse_rows[:, None] * inverse_cols[None, :]
            + damping * identity
        )
        result_tile = newton_steps(damped / divisor, identity)
        return lax.all_to_all(
            result_tile.astype(jnp.bfloat16), "blk", split_axis=0, concat_axis=1, tiled=True
        ).astype(result_tile.dtype)

    return inverse_tile(activations), inverse_tile(out_grads)


def cut(length, unit, pieces):
    units = length // unit
    sizes = [(units // pieces + (1 if i < units % pieces else 0)) * unit for i in range(pieces)]
    return [(sum(sizes[:i]), sizes[i]) for i in range(pieces)]


def swap_cut(length, unit, count):
    loads = np.full(count, (2.0**count - 0.5) / count)
    loads[-1] -= 0.5
    steps = np.array([[2.0 ** ((d - j) % count) for j in range(count)] for d in range(count)])
    ends = np.rint(np.cumsum(np.linalg.solve(steps, loads)) * (length // unit)).astype(int) * unit
    ends = [0] + [int(e) for e in ends]
    return [(a, e - a) for a, e in zip(ends, ends[1:])]


def gather_blocks(tok, blk, swaps, first, second, out, sems, halfway=None):
    send_sem, recv_sem, pass_send, pass_recv, swap_send, swap_recv, local_sem = sems
    t = lax.axis_index("tok")
    b = lax.axis_index("blk")
    half = blk // 2
    dims = []
    bit = 2
    while bit < tok:
        dims.append((bit, 0))
        bit *= 2
    bit = 1
    while bit < half:
        dims.append((0, bit))
        bit *= 2
    count = len(dims)
    rows, cols = first.shape
    if swaps:
        parts = [((o, n), (0, cols)) for o, n in (swap_cut if half > 1 else cut)(rows, 16, count)]
    else:
        parts = [((0, rows), (o, n)) for o, n in cut(cols, 128, count)]

    def flip(j, steps, tok_bits=0, blk_bits=0):
        for s in range(count):
            if steps >> s & 1:
                dt, db = dims[(j + s) % count]
                tok_bits ^= dt
                blk_bits ^= db
        return jnp.bitwise_xor(t, tok_bits), jnp.bitwise_xor(b, blk_bits)

    def place(q, part, owner):
        (r0, rn), (c0, cn) = parts[part]
        tt, bb = owner
        if q:
            bb = jnp.bitwise_xor(bb, half)
        if swaps:
            row, col = tt * rows + r0, bb * cols + c0
        else:
            row, col = (tt * blk + bb) * rows + r0, c0
        return out.at[
            pl.ds(pl.multiple_of(row, 16), rn), pl.ds(pl.multiple_of(col, 128), cn)
        ]

    def own(q, part):
        (r0, rn), (c0, cn) = parts[part]
        if q and swaps:
            return place(q, part, (t, b))
        return (second if q else first).at[pl.ds(r0, rn), pl.ds(c0, cn)]

    def hop(q, j, steps, s):
        src = own(q, j) if steps == 0 else place(q, j, flip(j, steps))
        index = (q * count + j) * 2**count + (steps | 1 << s)
        return pltpu.make_async_remote_copy(
            src_ref=src,
            dst_ref=place(q, j, flip(j, steps)),
            send_sem=send_sem.at[index],
            recv_sem=recv_sem.at[index],
            device_id=flip(j, 1 << s),
            device_id_type=MESH,
        )

    def arrival(q, j, steps):
        index = (q * count + j) * 2**count + steps
        where = place(q, j, flip(j, steps))
        return pltpu.make_async_remote_copy(
            src_ref=where,
            dst_ref=where,
            send_sem=send_sem.at[index],
            recv_sem=recv_sem.at[index],
            device_id=flip(j, 1),
            device_id_type=MESH,
        )

    def handed(q, j, steps, sender):
        index = (q * count + j) * 2**count + steps
        if sender:
            where = place(q, j, flip(j, steps))
            src = own(q, j) if steps == 0 else where
        else:
            where = place(q, j, flip(j, steps, 1))
            src = where
        return pltpu.make_async_remote_copy(
            src_ref=src,
            dst_ref=where,
            send_sem=pass_send.at[index],
            recv_sem=pass_recv.at[index],
            device_id=(jnp.bitwise_xor(t, 1), b),
            device_id_type=MESH,
        )

    across = (t, jnp.bitwise_xor(b, half))

    def swap(part, sender):
        (r0, rn), (c0, cn) = parts[part]
        if sender:
            src = second.at[pl.ds(r0, rn), pl.ds(c0, cn)]
            where = place(1, part, across)
        else:
            src = where = place(1, part, (t, b))
        return pltpu.make_async_remote_copy(
            src_ref=src,
            dst_ref=where,
            send_sem=swap_send.at[part],
            recv_sem=swap_recv.at[part],
            device_id=across,
            device_id_type=MESH,
        )

    barrier = pltpu.get_barrier_semaphore()
    peers = [flip(0, 1 << s) for s in range(count)] + [(jnp.bitwise_xor(t, 1), b), across]
    for peer in peers:
        pl.semaphore_signal(barrier, inc=1, device_id=peer, device_id_type=MESH)
    pl.semaphore_wait(barrier, len(peers))

    pending = []

    def start(copy):
        copy.start()
        pending.append(copy)

    def begin(q):
        for s in range(count):
            for j in range(count):
                if s == 0 and q and swaps:
                    swap(j, False).wait_recv()
                start(hop(q, j, 0, s))
        for j in range(count):
            start(handed(q, j, 0, True))

    def advance(q, p):
        for steps in range(2**p, 2 ** (p + 1)):
            for j in range(count):
                arrival(q, j, steps).wait_recv()
                for s in range(p + 1, count):
                    start(hop(q, j, steps, s))
                start(handed(q, j, steps, True))

    begin(0)
    if swaps:
        for part in range(count):
            start(swap(part, True))
    locals_ = []
    for q in range(1 if swaps else 2):
        for part in range(count):
            copy = pltpu.make_async_copy(
                own(q, part), place(q, part, (t, b)), local_sem.at[q * count + part]
            )
            copy.start()
            locals_.append(copy)
    for p in range(count - 1):
        advance(0, p)
    begin(1)
    advance(0, count - 1)
    for copy in locals_:
        copy.wait()

    def received(q):
        for j in range(count):
            for steps in range(2**count):
                handed(q, j, steps, False).wait_recv()

    if halfway is not None:
        received(0)
        halfway()
    for p in range(count):
        advance(1, p)
    if halfway is None:
        received(0)
    received(1)
    for copy in pending:
        copy.wait_send()


def gather_scratch(tok, blk):
    count = (tok // 2).bit_length() - 1 + (blk // 2).bit_length() - 1
    slots = 2 * count * 2**count
    return (
        [pltpu.SemaphoreType.DMA((slots,))] * 4
        + [pltpu.SemaphoreType.DMA((count,))] * 2
        + [pltpu.SemaphoreType.DMA((2 * count,))]
    )


def row_starts(tok, blk, rows):
    t = lax.axis_index("tok")
    b = lax.axis_index("blk")
    return [
        pl.multiple_of((t * blk + bb) * rows, LANES) for bb in (b, jnp.bitwise_xor(b, blk // 2))
    ]


def gram_kernel(tok, blk, first, second, gram, rounded, x, turned, *sems):
    tokens, width = x.shape
    rows = width // (tok * blk)
    gather_blocks(tok, blk, True, first, second, x, sems)
    step = first.shape[0]
    for s, start in enumerate(row_starts(tok, blk, rows)):

        @pl.loop(0, tokens // step)
        def _(i):
            at = pl.ds(pl.multiple_of(i * step, step), step)
            turned[s * rows : (s + 1) * rows, at] = x[at, pl.ds(start, rows)].T

    @pl.loop(0, width // CHUNK)
    def _(i):
        at = pl.ds(pl.multiple_of(i * CHUNK, CHUNK), CHUNK)
        product = jnp.dot(turned[...], x[:, at], preferred_element_type=jnp.float32)
        gram[:, at] = product
        rounded[:, at] = product.astype(jnp.bfloat16)


def newton_kernel(
    tok, blk, tokens, rounded, gram, kept, came, g, square, left, inverse, sent,
    out_sem, in_sem, *sems
):
    width = g.shape[1]
    rows = width // (tok * blk)
    t = lax.axis_index("tok")
    b = lax.axis_index("blk")
    starts = row_starts(tok, blk, rows)
    factor = 1.0 / (tokens * divisor)
    shift = damping / divisor
    eye = lax.broadcasted_iota(jnp.int32, (LANES, LANES), 0) == lax.broadcasted_iota(
        jnp.int32, (LANES, LANES), 1
    )

    inverse_rows = []
    for s, start in enumerate(starts):
        parts = []
        for r in range(0, rows, LANES):
            own = gram[s * rows + r : s * rows + r + LANES, pl.ds(start + r, LANES)]
            total = jnp.sum(jnp.where(eye, own, 0.0), axis=1, keepdims=True)
            parts.append(lax.rsqrt(total / tokens + epsilon))
        inverse_rows += parts
    inverse_rows = jnp.concatenate(inverse_rows, axis=0)

    def identity(first_col, size):
        col = first_col + lax.broadcasted_iota(jnp.int32, (rows, size), 1)
        row = lax.broadcasted_iota(jnp.int32, (rows, size), 0)
        return jnp.concatenate(
            [(col - start == row).astype(jnp.float32) for start in starts], axis=0
        )

    def scaled(first_col, size):
        at = pl.ds(first_col, size)
        return gram[:, at] * factor * inverse_rows * inverse[:, at] + shift * identity(
            first_col, size
        )

    half = blk // 2
    depth = half * rows

    def fold(side, add):
        places = [pl.multiple_of((i * blk + side * half) * rows, LANES) for i in range(tok)]
        for place in places:
            for r in range(0, depth, LANES):
                at = pl.ds(place + r, LANES)
                block = jnp.where(eye, g[at, at].astype(jnp.float32), 0.0)
                total = jnp.sum(block, axis=0, keepdims=True)
                inverse[:, at] = lax.rsqrt(total / tokens + epsilon)
            at = pl.ds(place, depth)
            left[:, at] = (scaled(place, depth) * inverse[:, at]).astype(jnp.bfloat16)

        @pl.loop(0, width // CHUNK)
        def _(i):
            at = pl.ds(pl.multiple_of(i * CHUNK, CHUNK), CHUNK)
            total = square[:, at] if add else jnp.zeros((2 * rows, CHUNK), jnp.float32)
            for place in places:
                deep = pl.ds(place, depth)
                total += jnp.dot(left[:, deep], g[deep, at], preferred_element_type=jnp.float32)
            square[:, at] = total

    side = b // half
    gather_blocks(
        tok, blk, False, rounded.at[pl.ds(0, rows)], rounded.at[pl.ds(rows, rows)], g, sems,
        lambda: fold(side, False),
    )
    fold(1 - side, True)

    @pl.loop(0, width // CHUNK)
    def _(i):
        start = pl.multiple_of(i * CHUNK, CHUNK)
        at = pl.ds(start, CHUNK)
        square[:, at] = square[:, at] * (inverse[:, at] * factor) + shift * scaled(start, CHUNK)
        left[:, at] = (square[:, at] * inverse[:, at]).astype(jnp.bfloat16)

    def swap(i):
        at = pl.ds(pl.multiple_of(i * CHUNK, CHUNK), CHUNK)
        return pltpu.make_async_remote_copy(
            src_ref=sent.at[:, at],
            dst_ref=came.at[:, at],
            send_sem=out_sem.at[i],
            recv_sem=in_sem.at[i],
            device_id=(t, jnp.bitwise_xor(b, blk // 2)),
            device_id_type=MESH,
        )

    steps = width // CHUNK

    def finish(i):
        at = pl.ds(pl.multiple_of(i * CHUNK, CHUNK), CHUNK)
        product = jnp.dot(left[...], g[:, at], preferred_element_type=jnp.float32)
        squared = square[:, at]
        cube = product * (inverse[:, at] * factor) + shift * squared
        start = pl.multiple_of(i * CHUNK, CHUNK)
        result = 4.0 * identity(start, CHUNK) - 6.0 * scaled(start, CHUNK) + 4.0 * squared - cube
        kept[:, at] = result[:rows]
        sent[:, at] = result[rows:].astype(jnp.bfloat16)

    finish(0)

    @pl.loop(1, steps)
    def _(i):
        finish(i)
        swap(i - 1).start()

    swap(steps - 1).start()

    @pl.loop(0, steps)
    def _(i):
        swap(i).wait_recv()
        swap(i).wait_send()


def call(kernel, outs, scratch, tok, blk, collective_id, *operands):
    return pl.pallas_call(
        kernel,
        out_shape=outs,
        in_specs=[pl.BlockSpec(memory_space=pltpu.VMEM)] * len(operands),
        out_specs=[pl.BlockSpec(memory_space=pltpu.VMEM)] * len(outs),
        scratch_shapes=scratch + gather_scratch(tok, blk),
        compiler_params=pltpu.CompilerParams(
            collective_id=collective_id, has_side_effects=True, vmem_limit_bytes=60 * 1024 * 1024
        ),
    )(*operands)


def split_body(tok, blk, activations, out_grads):
    tokens = activations.shape[0] * tok
    width = activations.shape[1] * blk
    rows = width // (tok * blk)
    low = lax.axis_index("blk") < blk // 2
    mine = jnp.where(low, activations, out_grads)
    other = jnp.where(low, out_grads, activations)
    steps = width // CHUNK
    gram, rounded = call(
        functools.partial(gram_kernel, tok, blk),
        [
            jax.ShapeDtypeStruct((2 * rows, width), jnp.float32),
            jax.ShapeDtypeStruct((2 * rows, width), jnp.bfloat16),
        ],
        [
            pltpu.VMEM((tokens, width), jnp.bfloat16),
            pltpu.VMEM((2 * rows, tokens), jnp.bfloat16),
        ],
        tok, blk, 0, mine, other,
    )
    kept, came = call(
        functools.partial(newton_kernel, tok, blk, tokens),
        [
            jax.ShapeDtypeStruct((rows, width), jnp.float32),
            jax.ShapeDtypeStruct((rows, width), jnp.bfloat16),
        ],
        [
            pltpu.VMEM((width, width), jnp.bfloat16),
            pltpu.VMEM((2 * rows, width), jnp.float32),
            pltpu.VMEM((2 * rows, width), jnp.bfloat16),
            pltpu.VMEM((1, width), jnp.float32),
            pltpu.VMEM((rows, width), jnp.bfloat16),
            pltpu.SemaphoreType.DMA((steps,)),
            pltpu.SemaphoreType.DMA((steps,)),
        ],
        tok, blk, 1, rounded, gram,
    )
    came = came.astype(jnp.float32)
    return jnp.where(low, kept, came), jnp.where(low, came, kept)


def solution(mesh):
    tok, blk = mesh.shape["tok"], mesh.shape["blk"]
    placed = (P("tok", "blk"), P("tok", "blk"))

    def body(activations, out_grads):
        tokens, width = activations.shape[0] * tok, activations.shape[1] * blk
        whole = max(tokens, width) * width * activations.dtype.itemsize
        powers = tok & (tok - 1) == 0 and blk & (blk - 1) == 0 and tok > 2 and blk > 1
        powers = powers and width % (tok * blk * LANES) == 0
        if whole <= gathered_budget and powers:
            return split_body(tok, blk, activations, out_grads)
        return tiled_body(activations, out_grads)

    return jax.shard_map(
        body,
        mesh=mesh,
        in_specs=placed,
        out_specs=(P(("tok", "blk"), None), P(("tok", "blk"), None)),
        check_vma=False,
    )
```
